64 devices in a mesh: rep: 8 (over x, y, core), dp: 8 (over z).
Axes of the slice: x: 2, y: 2, z: 8, core: 2. Of those that a mesh axis runs over, the one named last changes fastest.
The devices are a block of a 4x4x8 slice.
Arguments:
- g_w_gate: bfloat16 [64, 2, 512, 4096], P(('rep', 'dp')), parts along dimension 0
- g_w_up: bfloat16 [64, 2, 512, 4096], P(('rep', 'dp')), parts along dimension 0
- g_w_down: bfloat16 [64, 2, 4096, 512], P(('rep', 'dp')), parts along dimension 0
- w_gate: bfloat16 [2, 512, 4096], replicated
- w_up: bfloat16 [2, 512, 4096], replicated
- w_down: bfloat16 [2, 4096, 512], replicated
- m_w_gate: float32 [2, 512, 4096], P(None, 'dp')
- m_w_up: float32 [2, 512, 4096], P(None, 'dp')
- m_w_down: float32 [2, 4096, 512], P(None, 'dp')
- v_w_gate: float32 [2, 512, 4096], P(None, 'dp')
- v_w_up: float32 [2, 512, 4096], P(None, 'dp')
- v_w_down: float32 [2, 4096, 512], P(None, 'dp')
Outputs:
- output 1: bfloat16 [16, 512, 4096], P('rep'), parts along dimension 0
- output 2: bfloat16 [16, 512, 4096], P('rep'), parts along dimension 0
- output 3: bfloat16 [16, 4096, 512], P('rep'), parts along dimension 0
- output 4: float32 [16, 512, 4096], P('rep', 'dp'), parts along dimension 0
- output 5: float32 [16, 512, 4096], P('rep', 'dp'), parts along dimension 0
- output 6: float32 [16, 4096, 512], P('rep', 'dp'), parts along dimension 0
- output 7: float32 [16, 512, 4096], P('rep', 'dp'), parts along dimension 0
- output 8: float32 [16, 512, 4096], P('rep', 'dp'), parts along dimension 0
- output 9: float32 [16, 4096, 512], P('rep', 'dp'), parts along dimension 0
There are 8 independent parts. The reference program is written for one: setup_inputs(seed, part) draws one part's arguments, and reference() takes and returns one part's arrays. A program takes and returns all parts, laid end to end along the dimension named above; an argument that names none is the same for every part.
All inputs are finite; a program needn't handle non-finite values.
Results may differ from the reference program's by a relative error of at most 0.022.
Values are sent between devices in bfloat16 or wider.
A program may use at most 768 MiB of HBM per device.

```python
import jax
import jax.numpy as jnp
from jax import lax

DEVICES = 8
D = 512
FF = 4096
LAYERS = 2
NAMES = ("w_gate", "w_up", "w_down")
SHAPES = {"w_gate": (LAYERS, D, FF), "w_up": (LAYERS, D, FF), "w_down": (LAYERS, FF, D)}


def setup_inputs(seed: int = 0, part: int = 0) -> dict:
    kz, *keys = jax.random.split(jax.random.key(seed), 1 + 5 * len(NAMES))
    loud = 2.0 ** jax.random.uniform(kz, (), jnp.float32, -1.0, 1.0)
    drawn = {}
    for name, key, both in zip(NAMES, keys[:3], keys[3:6], strict=True):
        own = jax.random.normal(jax.random.fold_in(key, part), (DEVICES, *SHAPES[name]), jnp.float32)
        shared = jax.random.normal(jax.random.fold_in(both, part), SHAPES[name], jnp.float32)
        drawn["g_" + name] = (loud * (0.7 * shared / DEVICES + 0.7 * own * DEVICES**-0.5)).astype(jnp.bfloat16)
    for name, key in zip(NAMES, keys[6:9], strict=True):
        drawn[name] = (jax.random.normal(key, SHAPES[name], jnp.float32) * SHAPES[name][1] ** -0.5).astype(jnp.bfloat16)
    for name, key in zip(NAMES, keys[9:12], strict=True):
        drawn["m_" + name] = loud * 0.5 * jax.random.normal(key, SHAPES[name], jnp.float32)
    for name, key in zip(NAMES, keys[12:15], strict=True):
        drawn["v_" + name] = loud * loud * jax.random.uniform(key, SHAPES[name], jnp.float32, 0.5, 1.5)
    return drawn


def adamw(w, m, v, g):
    m = 0.9 * m + 0.1 * g
    v = 0.95 * v + 0.05 * g * g
    step = m * lax.rsqrt(v + 1e-8) + 0.1 * w
    return (w - 0.02 * step).astype(jnp.bfloat16), m, v


def clipped(gradients, sum_of_squares, count):
    factor = jnp.minimum(1.0, 0.5 * lax.rsqrt(sum_of_squares / count + 1e-30))
    return [g * factor for g in gradients]


def reference(g_w_gate, g_w_up, g_w_down, w_gate, w_up, w_down, m_w_gate, m_w_up, m_w_down, v_w_gate, v_w_up, v_w_down):
    def total(terms):
        return lax.scan(lambda so_far, term: (so_far + term.astype(jnp.float32), None), jnp.zeros(terms.shape[1:], jnp.float32), terms)[0]

    gradients = [total(terms).astype(jnp.bfloat16).astype(jnp.float32) for terms in (g_w_gate, g_w_up, g_w_down)]
    gradients = clipped(gradients, sum(jnp.sum(g * g) for g in gradients), sum(g.size for g in gradients))
    new = [
        adamw(w.astype(jnp.float32), m, v, g)
        for w, m, v, g in zip((w_gate, w_up, w_down), (m_w_gate, m_w_up, m_w_down), (v_w_gate, v_w_up, v_w_down), gradients, strict=True)
    ]
    return tuple(one[which] for which in range(3) for one in new)
```

```python
import functools

import jax
import jax.numpy as jnp
from jax import lax
from jax.experimental import pallas as pl
from jax.experimental.pallas import tpu as pltpu
from jax.sharding import PartitionSpec as P

MESH = pl.DeviceIdType.MESH
WAYS = 2


def adamw(w, m, v, g):
    m = 0.9 * m + 0.1 * g
    v = 0.95 * v + 0.05 * g * g
    step = m * lax.rsqrt(v + 1e-8) + 0.1 * w
    return (w - 0.02 * step).astype(jnp.bfloat16), m, v


def kernel(n, *refs):
    g, w, m, v = (refs[i : i + 3] for i in (0, 3, 6, 9))
    out, m_new, v_new = (refs[i : i + 3] for i in (12, 15, 18))
    terms, w_own = refs[21:24], refs[24:27]
    squares, send_sem, sum_sem, whole_sem, term_sem, own_sem, sq_send, sq_recv = refs[27:35]
    layers = out[0].shape[0]
    me = lax.axis_index("dp")
    chunks = [(which, layer) for which in range(3) for layer in range(layers)]
    own = [ref.shape[1] // n for ref in out]
    half = [rows // WAYS for rows in own]
    to = (lax.rem(me + 1, n), lax.rem(me + n - 1, n))
    sign = (1, -1)

    def rows(which, block, way):
        return pl.ds(pl.multiple_of(block * own[which] + way * half[which], half[which]), half[which])

    def block_of(way, back):
        return lax.rem(me - sign[way] * back + 2 * n, n)

    def term_copy(way, step, c):
        which, layer = chunks[c]
        slot = lax.rem(step, 2)
        return pltpu.make_async_copy(
            g[which].at[0, layer, rows(which, block_of(way, step + 2), way)],
            terms[which].at[way, slot, layer],
            term_sem.at[way, slot, c],
        )

    def send(way, c, src, place, sem):
        return pltpu.make_async_remote_copy(
            src_ref=src,
            dst_ref=place,
            send_sem=send_sem.at[way, c],
            recv_sem=sem,
            device_id={"dp": to[way]},
            device_id_type=MESH,
        )

    every = [(c, way) for c in range(len(chunks)) for way in range(WAYS)]

    for c, way in every:
        term_copy(way, 0, c).start()
    for c, way in every:
        term_copy(way, 1, c).start()
    barrier = pltpu.get_barrier_semaphore()
    for k in range(1, n):
        pl.semaphore_signal(barrier, inc=1, device_id={"dp": lax.rem(me + k, n)}, device_id_type=MESH)
    pl.semaphore_wait(barrier, n - 1)

    def sum_send(way, step, c):
        which, layer = chunks[c]
        place = out[which].at[layer, rows(which, block_of(way, step + 1), way)]
        return send(way, c, place, place, sum_sem.at[way, step, c])

    for c, way in every:
        which, layer = chunks[c]
        at = rows(which, block_of(way, 1), way)
        send(way, c, g[which].at[0, layer, at], out[which].at[layer, at], sum_sem.at[way, 0, c]).start()

    own_loads = []
    for which in range(3):
        mine = pl.ds(pl.multiple_of(me * own[which], own[which]), own[which])
        own_loads += [
            pltpu.make_async_copy(w[which].at[:, mine], w_own[which], own_sem.at[0, which]),
            pltpu.make_async_copy(m[which], m_new[which], own_sem.at[1, which]),
            pltpu.make_async_copy(v[which], v_new[which], own_sem.at[2, which]),
        ]
    for copy in own_loads:
        copy.start()

    def add(way, step, c):
        which, layer = chunks[c]
        place = out[which].at[layer, rows(which, block_of(way, step + 2), way)]
        send(way, c, place, place, sum_sem.at[way, step, c]).wait_recv()
        term_copy(way, step, c).wait()
        term = terms[which][way, lax.rem(step, 2), layer]
        total = (place[...].astype(jnp.float32) + term.astype(jnp.float32)).astype(jnp.bfloat16)
        place[...] = total
        return total

    def sum_step(step, _):
        for c, way in every:
            add(way, step, c)
            sum_send(way, step, c).wait_send()
            sum_send(way, step + 1, c).start()

            @pl.when(step + 2 <= n - 2)
            def _():
                term_copy(way, step + 2, c).start()

        return 0

    lax.fori_loop(0, n - 2, sum_step, 0)
    tile = jnp.zeros((8, 128), jnp.float32)
    for c, way in every:
        total = add(way, n - 2, c).astype(jnp.float32)
        square = total * total
        square = jnp.sum(square.reshape(square.shape[0] // 8, 8, square.shape[1]), axis=0)
        for i in range(square.shape[1] // 128):
            tile = tile + square[:, i * 128 : (i + 1) * 128]
    for c, way in every:
        sum_send(way, n - 2, c).wait_send()

    squares[me] = tile
    tells = [
        pltpu.make_async_remote_copy(
            src_ref=squares.at[me],
            dst_ref=squares.at[me],
            send_sem=sq_send.at[k - 1],
            recv_sem=sq_recv.at[k - 1],
            device_id={"dp": lax.rem(me + k, n)},
            device_id_type=MESH,
        )
        for k in range(1, n)
    ]
    for tell in tells:
        tell.start()
    for copy in own_loads:
        copy.wait()
    for k in range(1, n):
        theirs = squares.at[lax.rem(me + n - k, n)]
        pltpu.make_async_remote_copy(
            src_ref=theirs, dst_ref=theirs, send_sem=sq_send.at[k - 1], recv_sem=sq_recv.at[k - 1],
            device_id={"dp": lax.rem(me + k, n)}, device_id_type=MESH,
        ).wait_recv()
    count = n * sum(ref.size for ref in m)
    total = jnp.sum(jnp.sum(squares[...], axis=0), axis=(0, 1), keepdims=True)
    factor = jnp.minimum(1.0, 0.5 * lax.rsqrt(total / count + 1e-30))

    def whole_send(way, step, c):
        which, layer = chunks[c]
        place = out[which].at[layer, rows(which, block_of(way, step), way)]
        return send(way, c, place, place, whole_sem.at[way, step, c])

    for c, way in every:
        which, layer = chunks[c]
        here = pl.ds(way * half[which], half[which])
        place = out[which].at[layer, rows(which, me, way)]
        new = adamw(
            w_own[which][layer, here].astype(jnp.float32),
            m_new[which][layer, here],
            v_new[which][layer, here],
            place[...].astype(jnp.float32) * factor,
        )
        place[...], m_new[which][layer, here], v_new[which][layer, here] = new
        whole_send(way, 0, c).start()

    def arrived(way, step, c):
        which, layer = chunks[c]
        place = out[which].at[layer, rows(which, block_of(way, step + 1), way)]
        send(way, c, place, place, whole_sem.at[way, step, c]).wait_recv()

    def whole_step(step, _):
        for c, way in every:
            arrived(way, step, c)
            whole_send(way, step, c).wait_send()
            whole_send(way, step + 1, c).start()
        return 0

    lax.fori_loop(0, n - 2, whole_step, 0)
    for c, way in every:
        arrived(way, n - 2, c)
    for c, way in every:
        whole_send(way, n - 2, c).wait_send()
    for tell in tells:
        tell.wait_send()


def put_out(*refs):
    copies = [pltpu.make_async_copy(refs[i], refs[9 + i], refs[18].at[i]) for i in range(9)]
    for copy in copies:
        copy.start()
    for copy in copies:
        copy.wait()


def solution(mesh):
    n = mesh.shape["dp"]

    def step(*arrays):
        terms, weights, m, v = (arrays[i : i + 3] for i in (0, 3, 6, 9))
        layers = weights[0].shape[0]
        count = 3 * layers
        anywhere = pl.BlockSpec(memory_space=pl.ANY)
        half = [(x.shape[1] // n // WAYS, x.shape[2]) for x in weights]
        made = pl.pallas_call(
            functools.partial(kernel, n),
            out_shape=[pltpu.VMEM(x.shape, x.dtype) for x in (*weights, *m, *v)],
            in_specs=[anywhere] * 12,
            out_specs=[pl.BlockSpec(memory_space=pltpu.VMEM)] * 9,
            scratch_shapes=[
                *(pltpu.VMEM((WAYS, 2, layers, *h), jnp.bfloat16) for h in half),
                *(pltpu.VMEM((layers, x.shape[1] // n, x.shape[2]), jnp.bfloat16) for x in weights),
                pltpu.VMEM((n, 8, 128), jnp.float32),
                pltpu.SemaphoreType.DMA((WAYS, count)),
                pltpu.SemaphoreType.DMA((WAYS, n - 1, count)),
                pltpu.SemaphoreType.DMA((WAYS, n - 1, count)),
                pltpu.SemaphoreType.DMA((WAYS, 2, count)),
                pltpu.SemaphoreType.DMA((3, 3)),
                pltpu.SemaphoreType.DMA((n - 1,)),
                pltpu.SemaphoreType.DMA((n - 1,)),
            ],
            compiler_params=pltpu.CompilerParams(
                collective_id=0, has_side_effects=True, vmem_limit_bytes=16 * 2**20
            ),
            name="step_end",
        )(*terms, *weights, *m, *v)
        return pl.pallas_call(
            put_out,
            out_shape=[jax.ShapeDtypeStruct(x.shape, x.dtype) for x in (*weights, *m, *v)],
            in_specs=[pl.BlockSpec(memory_space=pltpu.VMEM)] * 9,
            out_specs=[anywhere] * 9,
            scratch_shapes=[pltpu.SemaphoreType.DMA((9,))],
            compiler_params=pltpu.CompilerParams(vmem_limit_bytes=16 * 2**20),
            name="put_out",
        )(*made)

    all_of, cut = P(None, None, None), P(None, "dp", None)
    return jax.shard_map(
        step,
        mesh=mesh,
        in_specs=(P(("rep", "dp"), None, None, None),) * 3 + (all_of,) * 3 + (cut,) * 6,
        out_specs=(P("rep", None, None),) * 3 + (P("rep", "dp", None),) * 6,
        check_vma=False,
    )
```

```python
import functools

import jax
import jax.numpy as jnp
from jax import lax
from jax.experimental import pallas as pl
from jax.experimental.pallas import tpu as pltpu
from jax.sharding import PartitionSpec as P

MESH = pl.DeviceIdType.MESH
WAYS = 2
PARTS = 2
LAG = 22000


def adamw(w, m, v, g):
    m = 0.9 * m + 0.1 * g
    v = 0.95 * v + 0.05 * g * g
    step = m * lax.rsqrt(v + 1e-8) + 0.1 * w
    return (w - 0.02 * step).astype(jnp.bfloat16), m, v


class Ring:
    def __init__(self, n):
        self.n, self.me = n, lax.axis_index("dp")
        self.to = (lax.rem(self.me + 1, n), lax.rem(self.me + n - 1, n))

    def block_of(self, way, back):
        return lax.rem(self.me + (-back, back)[way] + 2 * self.n, self.n)

    def send(self, way, src, place, send_sem, recv_sem):
        return pltpu.make_async_remote_copy(
            src_ref=src,
            dst_ref=place,
            send_sem=send_sem,
            recv_sem=recv_sem,
            device_id={"dp": self.to[way]},
            device_id_type=MESH,
        )


def gather(ring, every, place_of, send_sem, recv_sem):
    def forward(way, step, c):
        place = place_of(way, ring.block_of(way, step), c)
        return ring.send(way, place, place, send_sem.at[way, c], recv_sem.at[way, step, c])

    def arrived(way, step, c):
        place = place_of(way, ring.block_of(way, step + 1), c)
        ring.send(way, place, place, send_sem.at[way, c], recv_sem.at[way, step, c]).wait_recv()

    def one(step, _):
        for c, way in every:
            arrived(way, step, c)
            forward(way, step, c).wait_send()
            forward(way, step + 1, c).start()
        return 0

    last = ring.n - 2
    lax.fori_loop(0, last, one, 0)
    for c, way in every:
        arrived(way, last, c)
    for c, way in every:
        forward(way, last, c).wait_send()


def sum_and_step(n, *refs):
    g, w, m, v = (refs[i : i + 3] for i in (0, 3, 6, 9))
    gate, up, own_down = refs[12:15]
    m_new, v_new = refs[15:18], refs[18:21]
    down, terms, w_own = refs[21], refs[22:25], refs[25:28]
    squares, send_sem, sum_sem, whole_sem, term_sem, own_sem, sq_send, sq_recv = refs[28:36]
    out = (gate, up, down)
    layers = down.shape[0]
    ring = Ring(n)
    me, block_of = ring.me, ring.block_of
    chunks = [(which, layer) for which in range(3) for layer in range(layers)]
    every = [(c, way) for c in range(len(chunks)) for way in range(WAYS)]
    own = [ref.shape[1] // n for ref in out]
    half = [rows // WAYS for rows in own]

    def rows(which, block, way):
        return pl.ds(pl.multiple_of(block * own[which] + way * half[which], half[which]), half[which])

    def place_of(way, block, c):
        which, layer = chunks[c]
        return out[which].at[layer, rows(which, block, way)]

    def term_copy(way, step, c):
        which, layer = chunks[c]
        slot = lax.rem(step, 2)
        return pltpu.make_async_copy(
            g[which].at[0, layer, rows(which, block_of(way, step + 2), way)],
            terms[which].at[way, slot, layer],
            term_sem.at[way, slot, c],
        )

    for step in range(2):
        for c, way in every:
            term_copy(way, step, c).start()
    barrier = pltpu.get_barrier_semaphore()
    for k in range(1, n):
        pl.semaphore_signal(barrier, inc=1, device_id={"dp": lax.rem(me + k, n)}, device_id_type=MESH)
    pl.semaphore_wait(barrier, n - 1)
    pl.delay(lax.rem(lax.axis_index("rep"), 2) * LAG)

    def sum_send(way, step, c):
        place = place_of(way, block_of(way, step + 1), c)
        return ring.send(way, place, place, send_sem.at[way, c], sum_sem.at[way, step, c])

    for c, way in every:
        which, layer = chunks[c]
        block = block_of(way, 1)
        src = g[which].at[0, layer, rows(which, block, way)]
        ring.send(way, src, place_of(way, block, c), send_sem.at[way, c], sum_sem.at[way, 0, c]).start()

    own_loads = []
    for which in range(3):
        mine = pl.ds(pl.multiple_of(me * own[which], own[which]), own[which])
        own_loads += [
            pltpu.make_async_copy(w[which].at[:, mine], w_own[which], own_sem.at[0, which]),
            pltpu.make_async_copy(m[which], m_new[which], own_sem.at[1, which]),
            pltpu.make_async_copy(v[which], v_new[which], own_sem.at[2, which]),
        ]
    for copy in own_loads:
        copy.start()

    def add(way, step, c):
        which, layer = chunks[c]
        place = place_of(way, block_of(way, step + 2), c)
        ring.send(way, place, place, send_sem.at[way, c], sum_sem.at[way, step, c]).wait_recv()
        term_copy(way, step, c).wait()
        term = terms[which][way, lax.rem(step, 2), layer]
        total = (place[...].astype(jnp.float32) + term.astype(jnp.float32)).astype(jnp.bfloat16)
        place[...] = total
        return total

    def sum_step(step, _):
        for c, way in every:
            add(way, step, c)
            sum_send(way, step, c).wait_send()
            sum_send(way, step + 1, c).start()

            @pl.when(step + 2 <= n - 2)
            def _():
                term_copy(way, step + 2, c).start()

        return 0

    lax.fori_loop(0, n - 2, sum_step, 0)
    tile = jnp.zeros((8, 128), jnp.float32)
    for c, way in every:
        total = add(way, n - 2, c).astype(jnp.float32)
        square = total * total
        square = jnp.sum(square.reshape(square.shape[0] // 8, 8, square.shape[1]), axis=0)
        for i in range(square.shape[1] // 128):
            tile = tile + square[:, i * 128 : (i + 1) * 128]
    for c, way in every:
        sum_send(way, n - 2, c).wait_send()

    squares[me] = tile

    def tell(k, whose):
        return pltpu.make_async_remote_copy(
            src_ref=squares.at[whose],
            dst_ref=squares.at[whose],
            send_sem=sq_send.at[k - 1],
            recv_sem=sq_recv.at[k - 1],
            device_id={"dp": lax.rem(me + k, n)},
            device_id_type=MESH,
        )

    for k in range(1, n):
        tell(k, me).start()
    for copy in own_loads:
        copy.wait()
    for k in range(1, n):
        tell(k, lax.rem(me + n - k, n)).wait_recv()
    count = n * sum(ref.size for ref in m)
    total = jnp.sum(jnp.sum(squares[...], axis=0), axis=(0, 1), keepdims=True)
    factor = jnp.minimum(1.0, 0.5 * lax.rsqrt(total / count + 1e-30))

    gathered = [(c, way) for c, way in every if chunks[c][0] < 2]
    for c, way in every:
        which, layer = chunks[c]
        here = pl.ds(way * half[which], half[which])
        place = place_of(way, me, c)
        new, m_new[which][layer, here], v_new[which][layer, here] = adamw(
            w_own[which][layer, here].astype(jnp.float32),
            m_new[which][layer, here],
            v_new[which][layer, here],
            place[...].astype(jnp.float32) * factor,
        )
        if (c, way) in gathered:
            place[...] = new
            ring.send(way, place, place, send_sem.at[way, c], whole_sem.at[way, 0, c]).start()
        else:
            own_down[layer, here] = new
    gather(ring, gathered, place_of, send_sem, whole_sem)
    for k in range(1, n):
        tell(k, me).wait_send()


def gather_last(n, new, after, out, send_sem, recv_sem):
    del after
    ring = Ring(n)
    layers, own = new.shape[:2]
    size = own // WAYS // PARTS
    every = [(c, way) for c in range(layers * PARTS) for way in range(WAYS)]

    def place_of(way, block, c):
        first = block * own + (way * PARTS + c % PARTS) * size
        return out.at[c // PARTS, pl.ds(pl.multiple_of(first, size), size)]

    barrier = pltpu.get_barrier_semaphore()
    for to in ring.to:
        pl.semaphore_signal(barrier, inc=1, device_id={"dp": to}, device_id_type=MESH)
    pl.semaphore_wait(barrier, WAYS)
    for c, way in every:
        src = new.at[c // PARTS, pl.ds((way * PARTS + c % PARTS) * size, size)]
        ring.send(way, src, place_of(way, ring.me, c), send_sem.at[way, c], recv_sem.at[way, 0, c]).start()
    out[:, pl.ds(pl.multiple_of(ring.me * own, own), own)] = new[...]

    gather(ring, every, place_of, send_sem, recv_sem)


def put_out(arrays, *refs):
    sem = refs[-1]
    copies = [pltpu.make_async_copy(refs[i], refs[arrays + i], sem.at[i]) for i in range(arrays)]
    for copy in copies:
        copy.start()
    if len(refs) > 2 * arrays + 1:
        refs[2 * arrays][...] = jnp.zeros_like(refs[2 * arrays])
    for copy in copies:
        copy.wait()


def solution(mesh):
    n = mesh.shape["dp"]

    def step(*arrays):
        terms, weights, m, v = (arrays[i : i + 3] for i in (0, 3, 6, 9))
        layers = weights[0].shape[0]
        count = 3 * layers
        hbm = pl.BlockSpec(memory_space=pltpu.HBM)
        vmem = pl.BlockSpec(memory_space=pltpu.VMEM)
        cut = [(layers, x.shape[1] // n, x.shape[2]) for x in weights]
        half = [(rows // WAYS, columns) for _, rows, columns in cut]
        moments = [pltpu.VMEM(x.shape, x.dtype) for x in (*m, *v)]
        gate, up, own_down, *moments = pl.pallas_call(
            functools.partial(sum_and_step, n),
            out_shape=[
                *(pltpu.VMEM(x.shape, x.dtype) for x in weights[:2]),
                pltpu.VMEM(cut[2], weights[2].dtype),
                *moments,
            ],
            in_specs=[hbm] * 12,
            out_specs=[vmem] * 9,
            scratch_shapes=[
                pltpu.VMEM(weights[2].shape, jnp.bfloat16),
                *(pltpu.VMEM((WAYS, 2, layers, *h), jnp.bfloat16) for h in half),
                *(pltpu.VMEM(c, jnp.bfloat16) for c in cut),
                pltpu.VMEM((n, 8, 128), jnp.float32),
                pltpu.SemaphoreType.DMA((WAYS, count)),
                pltpu.SemaphoreType.DMA((WAYS, n - 1, count)),
                pltpu.SemaphoreType.DMA((WAYS, n - 1, count)),
                pltpu.SemaphoreType.DMA((WAYS, 2, count)),
                pltpu.SemaphoreType.DMA((3, 3)),
                pltpu.SemaphoreType.DMA((n - 1,)),
                pltpu.SemaphoreType.DMA((n - 1,)),
            ],
            compiler_params=pltpu.CompilerParams(
                collective_id=0, has_side_effects=True, vmem_limit_bytes=24 * 2**20
            ),
            name="sum_and_step",
        )(*terms, *weights, *m, *v)

        def put(limit, token, *some):
            return pl.pallas_call(
                functools.partial(put_out, len(some)),
                out_shape=[jax.ShapeDtypeStruct(x.shape, x.dtype) for x in some]
                + [jax.ShapeDtypeStruct((8, 128), jnp.float32)] * token,
                in_specs=[vmem] * len(some),
                out_specs=[hbm] * len(some) + [vmem] * token,
                scratch_shapes=[pltpu.SemaphoreType.DMA((len(some),))],
                compiler_params=pltpu.CompilerParams(vmem_limit_bytes=limit * 2**20),
                name="put_out",
            )(*some)

        gate, up, *moments, token = put(24, 1, gate, up, *moments)
        pieces = layers * PARTS
        down = pl.pallas_call(
            functools.partial(gather_last, n),
            out_shape=pltpu.VMEM(weights[2].shape, weights[2].dtype),
            in_specs=[vmem, vmem],
            out_specs=vmem,
            scratch_shapes=[
                pltpu.SemaphoreType.DMA((WAYS, pieces)),
                pltpu.SemaphoreType.DMA((WAYS, n - 1, pieces)),
            ],
            compiler_params=pltpu.CompilerParams(
                collective_id=1, has_side_effects=True, vmem_limit_bytes=24 * 2**20
            ),
            name="gather_last",
        )(own_down, token)
        (down,) = put(24, 0, down)
        return gate, up, down, *moments

    all_of, cut = P(None, None, None), P(None, "dp", None)
    return jax.shard_map(
        step,
        mesh=mesh,
        in_specs=(P(("rep", "dp"), None, None, None),) * 3 + (all_of,) * 3 + (cut,) * 6,
        out_specs=(P("rep", None, None),) * 3 + (P("rep", "dp", None),) * 6,
        check_vma=False,
    )
```

```python
import functools

import jax
import jax.numpy as jnp
from jax import lax
from jax.experimental import pallas as pl
from jax.experimental.pallas import tpu as pltpu
from jax.sharding import PartitionSpec as P

MESH = pl.DeviceIdType.MESH
WAYS = 2
PARTS = 2
LAG = 25000


def adamw(w, m, v, g):
    m = 0.9 * m + 0.1 * g
    v = 0.95 * v + 0.05 * g * g
    step = m * lax.rsqrt(v + 1e-8) + 0.1 * w
    return (w - 0.02 * step).astype(jnp.bfloat16), m, v


class Ring:
    def __init__(self, n):
        self.n, self.me = n, lax.axis_index("dp")
        self.to = (lax.rem(self.me + 1, n), lax.rem(self.me + n - 1, n))

    def block_of(self, way, back):
        return lax.rem(self.me + (-back, back)[way] + 2 * self.n, self.n)

    def send(self, way, src, place, send_sem, recv_sem):
        return pltpu.make_async_remote_copy(
            src_ref=src,
            dst_ref=place,
            send_sem=send_sem,
            recv_sem=recv_sem,
            device_id={"dp": self.to[way]},
            device_id_type=MESH,
        )


def gather(ring, every, place_of, send_sem, recv_sem):
    def forward(way, step, c):
        place = place_of(way, ring.block_of(way, step), c)
        return ring.send(way, place, place, send_sem.at[way, c], recv_sem.at[way, step, c])

    def arrived(way, step, c):
        place = place_of(way, ring.block_of(way, step + 1), c)
        ring.send(way, place, place, send_sem.at[way, c], recv_sem.at[way, step, c]).wait_recv()

    def one(step, _):
        for c, way in every:
            arrived(way, step, c)
            forward(way, step, c).wait_send()
            forward(way, step + 1, c).start()
        return 0

    last = ring.n - 2
    lax.fori_loop(0, last, one, 0)
    for c, way in every:
        arrived(way, last, c)
    for c, way in every:
        forward(way, last, c).wait_send()


def sum_and_step(n, *refs):
    g, w, m, v = (refs[i : i + 3] for i in (0, 3, 6, 9))
    gate, up, own_down = refs[12:15]
    m_new, v_new = refs[15:18], refs[18:21]
    down, terms, w_own = refs[21], refs[22:25], refs[25:28]
    squares, send_sem, sum_sem, whole_sem, term_sem, own_sem, sq_send, sq_recv = refs[28:36]
    out = (gate, up, down)
    layers = down.shape[0]
    ring = Ring(n)
    me, block_of = ring.me, ring.block_of
    chunks = [(which, layer) for which in range(3) for layer in range(layers)]
    every = [(c, way) for c in range(len(chunks)) for way in range(WAYS)]
    own = [ref.shape[1] // n for ref in out]
    half = [rows // WAYS for rows in own]

    def rows(which, block, way):
        return pl.ds(pl.multiple_of(block * own[which] + way * half[which], half[which]), half[which])

    def place_of(way, block, c):
        which, layer = chunks[c]
        return out[which].at[layer, rows(which, block, way)]

    def term_copy(way, step, c):
        which, layer = chunks[c]
        slot = lax.rem(step, 2)
        return pltpu.make_async_copy(
            g[which].at[0, layer, rows(which, block_of(way, step + 2), way)],
            terms[which].at[way, slot, layer],
            term_sem.at[way, slot, c],
        )

    barrier = pltpu.get_barrier_semaphore()
    for to in ring.to:
        pl.semaphore_signal(barrier, inc=1, device_id={"dp": to}, device_id_type=MESH)
    for c, way in every:
        term_copy(way, 0, c).start()
    pl.semaphore_wait(barrier, WAYS)
    pl.delay(lax.rem(lax.axis_index("rep"), 2) * LAG)

    def sum_send(way, step, c):
        place = place_of(way, block_of(way, step + 1), c)
        return ring.send(way, place, place, send_sem.at[way, c], sum_sem.at[way, step, c])

    for c, way in every:
        which, layer = chunks[c]
        block = block_of(way, 1)
        src = g[which].at[0, layer, rows(which, block, way)]
        ring.send(way, src, place_of(way, block, c), send_sem.at[way, c], sum_sem.at[way, 0, c]).start()

    for c, way in every:
        term_copy(way, 1, c).start()
    own_loads = []
    for which in range(3):
        mine = pl.ds(pl.multiple_of(me * own[which], own[which]), own[which])
        own_loads += [
            pltpu.make_async_copy(w[which].at[:, mine], w_own[which], own_sem.at[0, which]),
            pltpu.make_async_copy(m[which], m_new[which], own_sem.at[1, which]),
            pltpu.make_async_copy(v[which], v_new[which], own_sem.at[2, which]),
        ]
    for copy in own_loads:
        copy.start()

    def add(way, step, c):
        which, layer = chunks[c]
        place = place_of(way, block_of(way, step + 2), c)
        ring.send(way, place, place, send_sem.at[way, c], sum_sem.at[way, step, c]).wait_recv()
        term_copy(way, step, c).wait()
        term = terms[which][way, lax.rem(step, 2), layer]
        total = (place[...].astype(jnp.float32) + term.astype(jnp.float32)).astype(jnp.bfloat16)
        place[...] = total
        return total

    def sum_step(step, _):
        for c, way in every:
            add(way, step, c)
            sum_send(way, step, c).wait_send()
            sum_send(way, step + 1, c).start()

            @pl.when(step + 2 <= n - 2)
            def _():
                term_copy(way, step + 2, c).start()

        return 0

    lax.fori_loop(0, n - 2, sum_step, 0)
    tile = jnp.zeros((8, 128), jnp.float32)
    for c, way in every:
        total = add(way, n - 2, c).astype(jnp.float32)
        square = total * total
        square = jnp.sum(square.reshape(square.shape[0] // 8, 8, square.shape[1]), axis=0)
        for i in range(square.shape[1] // 128):
            tile = tile + square[:, i * 128 : (i + 1) * 128]
    for c, way in every:
        sum_send(way, n - 2, c).wait_send()

    squares[me] = tile
    hops = (n // 2, n - 1 - n // 2)

    def tell(way, step):
        place = squares.at[block_of(way, step)]
        return ring.send(way, place, place, sq_send.at[way, step], sq_recv.at[way, step])

    def told(way, step):
        place = squares.at[block_of(way, step + 1)]
        ring.send(way, place, place, sq_send.at[way, step], sq_recv.at[way, step]).wait_recv()

    for way in range(WAYS):
        tell(way, 0).start()
    for copy in own_loads:
        copy.wait()
    for step in range(max(hops)):
        for way in range(WAYS):
            if step < hops[way]:
                told(way, step)
            if step + 1 < hops[way]:
                tell(way, step + 1).start()
    count = n * sum(ref.size for ref in m)
    total = jnp.sum(jnp.sum(squares[...], axis=0), axis=(0, 1), keepdims=True)
    factor = jnp.minimum(1.0, 0.5 * lax.rsqrt(total / count + 1e-30))

    gathered = [(c, way) for c, way in every if chunks[c][0] < 2]
    for c, way in every:
        which, layer = chunks[c]
        here = pl.ds(way * half[which], half[which])
        place = place_of(way, me, c)
        new, m_new[which][layer, here], v_new[which][layer, here] = adamw(
            w_own[which][layer, here].astype(jnp.float32),
            m_new[which][layer, here],
            v_new[which][layer, here],
            place[...].astype(jnp.float32) * factor,
        )
        if (c, way) in gathered:
            place[...] = new
            ring.send(way, place, place, send_sem.at[way, c], whole_sem.at[way, 0, c]).start()
        else:
            own_down[layer, here] = new
    gather(ring, gathered, place_of, send_sem, whole_sem)
    for way in range(WAYS):
        for step in range(hops[way]):
            tell(way, step).wait_send()


def gather_last(n, new, after, out, send_sem, recv_sem):
    del after
    ring = Ring(n)
    layers, own = new.shape[:2]
    size = own // WAYS // PARTS
    every = [(c, way) for c in range(layers * PARTS) for way in range(WAYS)]

    def place_of(way, block, c):
        first = block * own + (way * PARTS + c % PARTS) * size
        return out.at[c // PARTS, pl.ds(pl.multiple_of(first, size), size)]

    barrier = pltpu.get_barrier_semaphore()
    for to in ring.to:
        pl.semaphore_signal(barrier, inc=1, device_id={"dp": to}, device_id_type=MESH)
    pl.semaphore_wait(barrier, WAYS)
    for c, way in every:
        src = new.at[c // PARTS, pl.ds((way * PARTS + c % PARTS) * size, size)]
        ring.send(way, src, place_of(way, ring.me, c), send_sem.at[way, c], recv_sem.at[way, 0, c]).start()
    out[:, pl.ds(pl.multiple_of(ring.me * own, own), own)] = new[...]

    gather(ring, every, place_of, send_sem, recv_sem)


def put_out(arrays, *refs):
    sem = refs[-1]
    copies = [pltpu.make_async_copy(refs[i], refs[arrays + i], sem.at[i]) for i in range(arrays)]
    for copy in copies:
        copy.start()
    if len(refs) > 2 * arrays + 1:
        refs[2 * arrays][...] = jnp.zeros_like(refs[2 * arrays])
    for copy in copies:
        copy.wait()


def solution(mesh):
    n = mesh.shape["dp"]

    def step(*arrays):
        terms, weights, m, v = (arrays[i : i + 3] for i in (0, 3, 6, 9))
        layers = weights[0].shape[0]
        count = 3 * layers
        hbm = pl.BlockSpec(memory_space=pltpu.HBM)
        vmem = pl.BlockSpec(memory_space=pltpu.VMEM)
        cut = [(layers, x.shape[1] // n, x.shape[2]) for x in weights]
        half = [(rows // WAYS, columns) for _, rows, columns in cut]
        moments = [pltpu.VMEM(x.shape, x.dtype) for x in (*m, *v)]
        gate, up, own_down, *moments = pl.pallas_call(
            functools.partial(sum_and_step, n),
            out_shape=[
                *(pltpu.VMEM(x.shape, x.dtype) for x in weights[:2]),
                pltpu.VMEM(cut[2], weights[2].dtype),
                *moments,
            ],
            in_specs=[hbm] * 12,
            out_specs=[vmem] * 9,
            scratch_shapes=[
                pltpu.VMEM(weights[2].shape, jnp.bfloat16),
                *(pltpu.VMEM((WAYS, 2, layers, *h), jnp.bfloat16) for h in half),
                *(pltpu.VMEM(c, jnp.bfloat16) for c in cut),
                pltpu.VMEM((n, 8, 128), jnp.float32),
                pltpu.SemaphoreType.DMA((WAYS, count)),
                pltpu.SemaphoreType.DMA((WAYS, n - 1, count)),
                pltpu.SemaphoreType.DMA((WAYS, n - 1, count)),
                pltpu.SemaphoreType.DMA((WAYS, 2, count)),
                pltpu.SemaphoreType.DMA((3, 3)),
                pltpu.SemaphoreType.DMA((WAYS, n - 1)),
                pltpu.SemaphoreType.DMA((WAYS, n - 1)),
            ],
            compiler_params=pltpu.CompilerParams(
                collective_id=0, has_side_effects=True, vmem_limit_bytes=24 * 2**20
            ),
            name="sum_and_step",
        )(*terms, *weights, *m, *v)

        def put(limit, token, *some):
            return pl.pallas_call(
                functools.partial(put_out, len(some)),
                out_shape=[jax.ShapeDtypeStruct(x.shape, x.dtype) for x in some]
                + [jax.ShapeDtypeStruct((8, 128), jnp.float32)] * token,
                in_specs=[vmem] * len(some),
                out_specs=[hbm] * len(some) + [vmem] * token,
                scratch_shapes=[pltpu.SemaphoreType.DMA((len(some),))],
                compiler_params=pltpu.CompilerParams(vmem_limit_bytes=limit * 2**20),
                name="put_out",
            )(*some)

        gate, up, *moments, token = put(24, 1, gate, up, *moments)
        pieces = layers * PARTS
        down = pl.pallas_call(
            functools.partial(gather_last, n),
            out_shape=pltpu.VMEM(weights[2].shape, weights[2].dtype),
            in_specs=[vmem, vmem],
            out_specs=vmem,
            scratch_shapes=[
                pltpu.SemaphoreType.DMA((WAYS, pieces)),
                pltpu.SemaphoreType.DMA((WAYS, n - 1, pieces)),
            ],
            compiler_params=pltpu.CompilerParams(
                collective_id=1, has_side_effects=True, vmem_limit_bytes=24 * 2**20
            ),
            name="gather_last",
        )(own_down, token)
        (down,) = put(24, 0, down)
        return gate, up, down, *moments

    all_of, cut = P(None, None, None), P(None, "dp", None)
    return jax.shard_map(
        step,
        mesh=mesh,
        in_specs=(P(("rep", "dp"), None, None, None),) * 3 + (all_of,) * 3 + (cut,) * 6,
        out_specs=(P("rep", None, None),) * 3 + (P("rep", "dp", None),) * 6,
        check_vma=False,
    )
```

```python
import functools

import jax
import jax.numpy as jnp
from jax import lax
from jax.experimental import pallas as pl
from jax.experimental.pallas import tpu as pltpu
from jax.sharding import PartitionSpec as P

MESH = pl.DeviceIdType.MESH
WAYS = 2
PARTS = 1
LAG = 25000


def adamw(w, m, v, g):
    m = 0.9 * m + 0.1 * g
    v = 0.95 * v + 0.05 * g * g
    step = m * lax.rsqrt(v + 1e-8) + 0.1 * w
    return (w - 0.02 * step).astype(jnp.bfloat16), m, v


class Ring:
    def __init__(self, n):
        self.n, self.me = n, lax.axis_index("dp")
        self.to = (lax.rem(self.me + 1, n), lax.rem(self.me + n - 1, n))

    def block_of(self, way, back):
        return lax.rem(self.me + (-back, back)[way] + 2 * self.n, self.n)

    def send(self, way, src, place, send_sem, recv_sem):
        return pltpu.make_async_remote_copy(
            src_ref=src,
            dst_ref=place,
            send_sem=send_sem,
            recv_sem=recv_sem,
            device_id={"dp": self.to[way]},
            device_id_type=MESH,
        )


def gather(ring, every, place_of, send_sem, recv_sem):
    def forward(way, step, c):
        place = place_of(way, ring.block_of(way, step), c)
        return ring.send(way, place, place, send_sem.at[way, c], recv_sem.at[way, step, c])

    def arrived(way, step, c):
        place = place_of(way, ring.block_of(way, step + 1), c)
        ring.send(way, place, place, send_sem.at[way, c], recv_sem.at[way, step, c]).wait_recv()

    def one(step, _):
        for c, way in every:
            arrived(way, step, c)
            forward(way, step, c).wait_send()
            forward(way, step + 1, c).start()
        return 0

    last = ring.n - 2
    lax.fori_loop(0, last, one, 0)
    for c, way in every:
        arrived(way, last, c)
    for c, way in every:
        forward(way, last, c).wait_send()


def sum_and_step(n, *refs):
    g, w, m, v = (refs[i : i + 3] for i in (0, 3, 6, 9))
    gate, up, own_down = refs[12:15]
    m_new, v_new = refs[15:18], refs[18:21]
    down, terms, w_own = refs[21], refs[22:25], refs[25:28]
    squares, send_sem, sum_sem, whole_sem, term_sem, own_sem, sq_send, sq_recv = refs[28:36]
    out = (gate, up, down)
    ring = Ring(n)
    me, block_of = ring.me, ring.block_of
    every = [(c, way) for c in range(len(out)) for way in range(WAYS)]
    own = [ref.shape[1] // n for ref in out]
    half = [rows // WAYS for rows in own]

    def rows(which, block, way):
        return pl.ds(pl.multiple_of(block * own[which] + way * half[which], half[which]), half[which])

    def place_of(way, block, c):
        return out[c].at[:, rows(c, block, way)]

    def term_copy(way, step, c):
        slot = lax.rem(step, 2)
        return pltpu.make_async_copy(
            g[c].at[0, :, rows(c, block_of(way, step + 2), way)],
            terms[c].at[way, slot],
            term_sem.at[way, slot, c],
        )

    barrier = pltpu.get_barrier_semaphore()
    for to in ring.to:
        pl.semaphore_signal(barrier, inc=1, device_id={"dp": to}, device_id_type=MESH)
    for c, way in every:
        term_copy(way, 0, c).start()
    pl.semaphore_wait(barrier, WAYS)
    pl.delay(lax.rem(lax.axis_index("rep"), 2) * LAG)

    def sum_send(way, step, c):
        place = place_of(way, block_of(way, step + 1), c)
        return ring.send(way, place, place, send_sem.at[way, c], sum_sem.at[way, step, c])

    for c, way in every:
        block = block_of(way, 1)
        src = g[c].at[0, :, rows(c, block, way)]
        ring.send(way, src, place_of(way, block, c), send_sem.at[way, c], sum_sem.at[way, 0, c]).start()

    for c, way in every:
        term_copy(way, 1, c).start()
    own_loads = []
    for which in range(3):
        mine = pl.ds(pl.multiple_of(me * own[which], own[which]), own[which])
        own_loads += [
            pltpu.make_async_copy(w[which].at[:, mine], w_own[which], own_sem.at[0, which]),
            pltpu.make_async_copy(m[which], m_new[which], own_sem.at[1, which]),
            pltpu.make_async_copy(v[which], v_new[which], own_sem.at[2, which]),
        ]
    for copy in own_loads:
        copy.start()

    def add(way, step, c):
        place = place_of(way, block_of(way, step + 2), c)
        ring.send(way, place, place, send_sem.at[way, c], sum_sem.at[way, step, c]).wait_recv()
        term_copy(way, step, c).wait()
        term = terms[c][way, lax.rem(step, 2)]
        total = (place[...].astype(jnp.float32) + term.astype(jnp.float32)).astype(jnp.bfloat16)
        place[...] = total
        return total

    def sum_step(step, _):
        for c, way in every:
            add(way, step, c)
            sum_send(way, step, c).wait_send()
            sum_send(way, step + 1, c).start()

            @pl.when(step + 2 <= n - 2)
            def _():
                term_copy(way, step + 2, c).start()

        return 0

    lax.fori_loop(0, n - 2, sum_step, 0)
    tile = jnp.zeros((8, 128), jnp.float32)
    for c, way in every:
        total = add(way, n - 2, c).astype(jnp.float32)
        square = total * total
        square = jnp.sum(square.reshape(-1, 8, square.shape[-1]), axis=0)
        for i in range(square.shape[1] // 128):
            tile = tile + square[:, i * 128 : (i + 1) * 128]
    for c, way in every:
        sum_send(way, n - 2, c).wait_send()

    squares[me] = tile
    hops = (n // 2, n - 1 - n // 2)

    def tell(way, step):
        place = squares.at[block_of(way, step)]
        return ring.send(way, place, place, sq_send.at[way, step], sq_recv.at[way, step])

    def told(way, step):
        place = squares.at[block_of(way, step + 1)]
        ring.send(way, place, place, sq_send.at[way, step], sq_recv.at[way, step]).wait_recv()

    for way in range(WAYS):
        tell(way, 0).start()
    for copy in own_loads:
        copy.wait()
    for step in range(max(hops)):
        for way in range(WAYS):
            if step < hops[way]:
                told(way, step)
            if step + 1 < hops[way]:
                tell(way, step + 1).start()
    count = n * sum(ref.size for ref in m)
    total = jnp.sum(jnp.sum(squares[...], axis=0), axis=(0, 1), keepdims=True)
    factor = jnp.minimum(1.0, 0.5 * lax.rsqrt(total / count + 1e-30))

    gathered = [(c, way) for c, way in every if c < 2]
    for c, way in every:
        here = pl.ds(way * half[c], half[c])
        place = place_of(way, me, c)
        new, m_new[c][:, here], v_new[c][:, here] = adamw(
            w_own[c][:, here].astype(jnp.float32),
            m_new[c][:, here],
            v_new[c][:, here],
            place[...].astype(jnp.float32) * factor,
        )
        if (c, way) in gathered:
            place[...] = new
            ring.send(way, place, place, send_sem.at[way, c], whole_sem.at[way, 0, c]).start()
        else:
            own_down[:, here] = new
    gather(ring, gathered, place_of, send_sem, whole_sem)
    for way in range(WAYS):
        for step in range(hops[way]):
            tell(way, step).wait_send()


def gather_last(n, new, after, out, send_sem, recv_sem):
    del after
    ring = Ring(n)
    layers, own = new.shape[:2]
    size = own // WAYS // PARTS
    every = [(c, way) for c in range(layers * PARTS) for way in range(WAYS)]

    def place_of(way, block, c):
        first = block * own + (way * PARTS + c % PARTS) * size
        return out.at[c // PARTS, pl.ds(pl.multiple_of(first, size), size)]

    barrier = pltpu.get_barrier_semaphore()
    for to in ring.to:
        pl.semaphore_signal(barrier, inc=1, device_id={"dp": to}, device_id_type=MESH)
    pl.semaphore_wait(barrier, WAYS)
    for c, way in every:
        src = new.at[c // PARTS, pl.ds((way * PARTS + c % PARTS) * size, size)]
        ring.send(way, src, place_of(way, ring.me, c), send_sem.at[way, c], recv_sem.at[way, 0, c]).start()
    out[:, pl.ds(pl.multiple_of(ring.me * own, own), own)] = new[...]

    gather(ring, every, place_of, send_sem, recv_sem)


def put_out(arrays, *refs):
    sem = refs[-1]
    copies = [pltpu.make_async_copy(refs[i], refs[arrays + i], sem.at[i]) for i in range(arrays)]
    for copy in copies:
        copy.start()
    if len(refs) > 2 * arrays + 1:
        refs[2 * arrays][...] = jnp.zeros_like(refs[2 * arrays])
    for copy in copies:
        copy.wait()


def solution(mesh):
    n = mesh.shape["dp"]

    def step(*arrays):
        terms, weights, m, v = (arrays[i : i + 3] for i in (0, 3, 6, 9))
        layers = weights[0].shape[0]
        count = len(weights)
        hbm = pl.BlockSpec(memory_space=pltpu.HBM)
        vmem = pl.BlockSpec(memory_space=pltpu.VMEM)
        cut = [(layers, x.shape[1] // n, x.shape[2]) for x in weights]
        half = [(rows // WAYS, columns) for _, rows, columns in cut]
        moments = [pltpu.VMEM(x.shape, x.dtype) for x in (*m, *v)]
        gate, up, own_down, *moments = pl.pallas_call(
            functools.partial(sum_and_step, n),
            out_shape=[
                *(pltpu.VMEM(x.shape, x.dtype) for x in weights[:2]),
                pltpu.VMEM(cut[2], weights[2].dtype),
                *moments,
            ],
            in_specs=[hbm] * 12,
            out_specs=[vmem] * 9,
            scratch_shapes=[
                pltpu.VMEM(weights[2].shape, jnp.bfloat16),
                *(pltpu.VMEM((WAYS, 2, layers, *h), jnp.bfloat16) for h in half),
                *(pltpu.VMEM(c, jnp.bfloat16) for c in cut),
                pltpu.VMEM((n, 8, 128), jnp.float32),
                pltpu.SemaphoreType.DMA((WAYS, count)),
                pltpu.SemaphoreType.DMA((WAYS, n - 1, count)),
                pltpu.SemaphoreType.DMA((WAYS, n - 1, count)),
                pltpu.SemaphoreType.DMA((WAYS, 2, count)),
                pltpu.SemaphoreType.DMA((3, 3)),
                pltpu.SemaphoreType.DMA((WAYS, n - 1)),
                pltpu.SemaphoreType.DMA((WAYS, n - 1)),
            ],
            compiler_params=pltpu.CompilerParams(
                collective_id=0, has_side_effects=True, vmem_limit_bytes=24 * 2**20
            ),
            name="sum_and_step",
        )(*terms, *weights, *m, *v)

        def put(limit, token, *some):
            return pl.pallas_call(
                functools.partial(put_out, len(some)),
                out_shape=[jax.ShapeDtypeStruct(x.shape, x.dtype) for x in some]
                + [jax.ShapeDtypeStruct((8, 128), jnp.float32)] * token,
                in_specs=[vmem] * len(some),
                out_specs=[hbm] * len(some) + [vmem] * token,
                scratch_shapes=[pltpu.SemaphoreType.DMA((len(some),))],
                compiler_params=pltpu.CompilerParams(vmem_limit_bytes=limit * 2**20),
                name="put_out",
            )(*some)

        gate, up, *moments, token = put(24, 1, gate, up, *moments)
        pieces = layers * PARTS
        down = pl.pallas_call(
            functools.partial(gather_last, n),
            out_shape=pltpu.VMEM(weights[2].shape, weights[2].dtype),
            in_specs=[vmem, vmem],
            out_specs=vmem,
            scratch_shapes=[
                pltpu.SemaphoreType.DMA((WAYS, pieces)),
                pltpu.SemaphoreType.DMA((WAYS, n - 1, pieces)),
            ],
            compiler_params=pltpu.CompilerParams(
                collective_id=1, has_side_effects=True, vmem_limit_bytes=24 * 2**20
            ),
            name="gather_last",
        )(own_down, token)
        (down,) = put(24, 0, down)
        return gate, up, down, *moments

    all_of, cut = P(None, None, None), P(None, "dp", None)
    return jax.shard_map(
        step,
        mesh=mesh,
        in_specs=(P(("rep", "dp"), None, None, None),) * 3 + (all_of,) * 3 + (cut,) * 6,
        out_specs=(P("rep", None, None),) * 3 + (P("rep", "dp", None),) * 6,
        check_vma=False,
    )
```

```python
import functools

import jax
import jax.numpy as jnp
from jax import lax
from jax.experimental import pallas as pl
from jax.experimental.pallas import tpu as pltpu
from jax.sharding import PartitionSpec as P

MESH = pl.DeviceIdType.MESH
WAYS = 2
PARTS = 1
LAG = 25000


def adamw(w, m, v, g):
    m = 0.9 * m + 0.1 * g
    v = 0.95 * v + 0.05 * g * g
    step = m * lax.rsqrt(v + 1e-8) + 0.1 * w
    return (w - 0.02 * step).astype(jnp.bfloat16), m, v


class Ring:
    def __init__(self, n):
        self.n, self.me = n, lax.axis_index("dp")
        self.to = (lax.rem(self.me + 1, n), lax.rem(self.me + n - 1, n))

    def block_of(self, way, back):
        return lax.rem(self.me + (-back, back)[way] + 2 * self.n, self.n)

    def send(self, way, src, place, send_sem, recv_sem):
        return pltpu.make_async_remote_copy(
            src_ref=src,
            dst_ref=place,
            send_sem=send_sem,
            recv_sem=recv_sem,
            device_id={"dp": self.to[way]},
            device_id_type=MESH,
        )


def gather(ring, every, place_of, send_sem, recv_sem):
    def forward(way, step, c):
        place = place_of(way, ring.block_of(way, step), c)
        return ring.send(way, place, place, send_sem.at[way, c], recv_sem.at[way, step, c])

    def arrived(way, step, c):
        place = place_of(way, ring.block_of(way, step + 1), c)
        ring.send(way, place, place, send_sem.at[way, c], recv_sem.at[way, step, c]).wait_recv()

    def one(step, _):
        for c, way in every:
            arrived(way, step, c)
            forward(way, step, c).wait_send()
            forward(way, step + 1, c).start()
        return 0

    last = ring.n - 2
    lax.fori_loop(0, last, one, 0)
    for c, way in every:
        arrived(way, last, c)
    for c, way in every:
        forward(way, last, c).wait_send()


def sum_and_step(n, *refs):
    g, w, m, v = (refs[i : i + 3] for i in (0, 3, 6, 9))
    gate, up, own_down = refs[12:15]
    m_new, v_new = refs[15:18], refs[18:21]
    down, terms, w_own = refs[21], refs[22:25], refs[25:28]
    squares, send_sem, sum_sem, whole_sem, term_sem, own_sem, sq_send, sq_recv = refs[28:36]
    out = (gate, up, down)
    ring = Ring(n)
    me, block_of = ring.me, ring.block_of
    every = [(c, way) for c in range(len(out)) for way in range(WAYS)]
    own = [ref.shape[1] // n for ref in out]
    half = [rows // WAYS for rows in own]

    def rows(which, block, way):
        return pl.ds(pl.multiple_of(block * own[which] + way * half[which], half[which]), half[which])

    def place_of(way, block, c):
        return out[c].at[:, rows(c, block, way)]

    def term_copy(way, step, c):
        slot = lax.rem(step, 2)
        return pltpu.make_async_copy(
            g[c].at[0, :, rows(c, block_of(way, step + 2), way)],
            terms[c].at[way, slot],
            term_sem.at[way, slot, c],
        )

    barrier = pltpu.get_barrier_semaphore()
    for to in ring.to:
        pl.semaphore_signal(barrier, inc=1, device_id={"dp": to}, device_id_type=MESH)
    pl.semaphore_wait(barrier, WAYS)
    pl.delay(lax.rem(lax.axis_index("rep"), 2) * LAG)

    def sum_send(way, step, c):
        place = place_of(way, block_of(way, step + 1), c)
        return ring.send(way, place, place, send_sem.at[way, c], sum_sem.at[way, step, c])

    for c, way in every:
        block = block_of(way, 1)
        src = g[c].at[0, :, rows(c, block, way)]
        ring.send(way, src, place_of(way, block, c), send_sem.at[way, c], sum_sem.at[way, 0, c]).start()

    for step in range(2):
        for c, way in every:
            term_copy(way, step, c).start()
    own_loads = []
    for which in range(3):
        mine = pl.ds(pl.multiple_of(me * own[which], own[which]), own[which])
        own_loads += [
            pltpu.make_async_copy(w[which].at[:, mine], w_own[which], own_sem.at[0, which]),
            pltpu.make_async_copy(m[which], m_new[which], own_sem.at[1, which]),
            pltpu.make_async_copy(v[which], v_new[which], own_sem.at[2, which]),
        ]
    for copy in own_loads:
        copy.start()

    def add(way, step, c):
        place = place_of(way, block_of(way, step + 2), c)
        ring.send(way, place, place, send_sem.at[way, c], sum_sem.at[way, step, c]).wait_recv()
        term_copy(way, step, c).wait()
        term = terms[c][way, lax.rem(step, 2)]
        total = (place[...].astype(jnp.float32) + term.astype(jnp.float32)).astype(jnp.bfloat16)
        place[...] = total
        return total

    def sum_step(step, _):
        for c, way in every:
            add(way, step, c)
            sum_send(way, step, c).wait_send()
            sum_send(way, step + 1, c).start()

            @pl.when(step + 2 <= n - 2)
            def _():
                term_copy(way, step + 2, c).start()

        return 0

    lax.fori_loop(0, n - 2, sum_step, 0)
    tile = jnp.zeros((8, 128), jnp.float32)
    for c, way in every:
        total = add(way, n - 2, c).astype(jnp.float32)
        square = total * total
        square = jnp.sum(square.reshape(-1, 8, square.shape[-1]), axis=0)
        for i in range(square.shape[1] // 128):
            tile = tile + square[:, i * 128 : (i + 1) * 128]
    for c, way in every:
        sum_send(way, n - 2, c).wait_send()

    squares[me] = tile
    hops = (n // 2, n - 1 - n // 2)

    def tell(way, step):
        place = squares.at[block_of(way, step)]
        return ring.send(way, place, place, sq_send.at[way, step], sq_recv.at[way, step])

    def told(way, step):
        place = squares.at[block_of(way, step + 1)]
        ring.send(way, place, place, sq_send.at[way, step], sq_recv.at[way, step]).wait_recv()

    for way in range(WAYS):
        tell(way, 0).start()
    for copy in own_loads:
        copy.wait()
    for step in range(max(hops)):
        for way in range(WAYS):
            if step < hops[way]:
                told(way, step)
            if step + 1 < hops[way]:
                tell(way, step + 1).start()
    count = n * sum(ref.size for ref in m)
    total = jnp.sum(jnp.sum(squares[...], axis=0), axis=(0, 1), keepdims=True)
    factor = jnp.minimum(1.0, 0.5 * lax.rsqrt(total / count + 1e-30))

    gathered = [(c, way) for c, way in every if c < 2]
    for c, way in every:
        here = pl.ds(way * half[c], half[c])
        place = place_of(way, me, c)
        new, m_new[c][:, here], v_new[c][:, here] = adamw(
            w_own[c][:, here].astype(jnp.float32),
            m_new[c][:, here],
            v_new[c][:, here],
            place[...].astype(jnp.float32) * factor,
        )
        if (c, way) in gathered:
            place[...] = new
            ring.send(way, place, place, send_sem.at[way, c], whole_sem.at[way, 0, c]).start()
        else:
            own_down[:, here] = new
    gather(ring, gathered, place_of, send_sem, whole_sem)
    for way in range(WAYS):
        for step in range(hops[way]):
            tell(way, step).wait_send()


def gather_last(n, new, after, out, send_sem, recv_sem):
    del after
    ring = Ring(n)
    layers, own = new.shape[:2]
    size = own // WAYS // PARTS
    every = [(c, way) for c in range(layers * PARTS) for way in range(WAYS)]

    def place_of(way, block, c):
        first = block * own + (way * PARTS + c % PARTS) * size
        return out.at[c // PARTS, pl.ds(pl.multiple_of(first, size), size)]

    barrier = pltpu.get_barrier_semaphore()
    for to in ring.to:
        pl.semaphore_signal(barrier, inc=1, device_id={"dp": to}, device_id_type=MESH)
    pl.semaphore_wait(barrier, WAYS)
    for c, way in every:
        src = new.at[c // PARTS, pl.ds((way * PARTS + c % PARTS) * size, size)]
        ring.send(way, src, place_of(way, ring.me, c), send_sem.at[way, c], recv_sem.at[way, 0, c]).start()
    out[:, pl.ds(pl.multiple_of(ring.me * own, own), own)] = new[...]

    gather(ring, every, place_of, send_sem, recv_sem)


def put_out(arrays, *refs):
    sem = refs[-1]
    copies = [pltpu.make_async_copy(refs[i], refs[arrays + i], sem.at[i]) for i in range(arrays)]
    for copy in copies:
        copy.start()
    if len(refs) > 2 * arrays + 1:
        refs[2 * arrays][...] = jnp.zeros_like(refs[2 * arrays])
    for copy in copies:
        copy.wait()


def solution(mesh):
    n = mesh.shape["dp"]

    def step(*arrays):
        terms, weights, m, v = (arrays[i : i + 3] for i in (0, 3, 6, 9))
        layers = weights[0].shape[0]
        count = len(weights)
        hbm = pl.BlockSpec(memory_space=pltpu.HBM)
        vmem = pl.BlockSpec(memory_space=pltpu.VMEM)
        cut = [(layers, x.shape[1] // n, x.shape[2]) for x in weights]
        half = [(rows // WAYS, columns) for _, rows, columns in cut]
        moments = [pltpu.VMEM(x.shape, x.dtype) for x in (*m, *v)]
        gate, up, own_down, *moments = pl.pallas_call(
            functools.partial(sum_and_step, n),
            out_shape=[
                *(pltpu.VMEM(x.shape, x.dtype) for x in weights[:2]),
                pltpu.VMEM(cut[2], weights[2].dtype),
                *moments,
            ],
            in_specs=[hbm] * 12,
            out_specs=[vmem] * 9,
            scratch_shapes=[
                pltpu.VMEM(weights[2].shape, jnp.bfloat16),
                *(pltpu.VMEM((WAYS, 2, layers, *h), jnp.bfloat16) for h in half),
                *(pltpu.VMEM(c, jnp.bfloat16) for c in cut),
                pltpu.VMEM((n, 8, 128), jnp.float32),
                pltpu.SemaphoreType.DMA((WAYS, count)),
                pltpu.SemaphoreType.DMA((WAYS, n - 1, count)),
                pltpu.SemaphoreType.DMA((WAYS, n - 1, count)),
                pltpu.SemaphoreType.DMA((WAYS, 2, count)),
                pltpu.SemaphoreType.DMA((3, 3)),
                pltpu.SemaphoreType.DMA((WAYS, n - 1)),
                pltpu.SemaphoreType.DMA((WAYS, n - 1)),
            ],
            compiler_params=pltpu.CompilerParams(
                collective_id=0, has_side_effects=True, vmem_limit_bytes=24 * 2**20
            ),
            name="sum_and_step",
        )(*terms, *weights, *m, *v)

        def put(limit, token, *some):
            return pl.pallas_call(
                functools.partial(put_out, len(some)),
                out_shape=[jax.ShapeDtypeStruct(x.shape, x.dtype) for x in some]
                + [jax.ShapeDtypeStruct((8, 128), jnp.float32)] * token,
                in_specs=[vmem] * len(some),
                out_specs=[hbm] * len(some) + [vmem] * token,
                scratch_shapes=[pltpu.SemaphoreType.DMA((len(some),))],
                compiler_params=pltpu.CompilerParams(vmem_limit_bytes=limit * 2**20),
                name="put_out",
            )(*some)

        gate, up, *moments, token = put(24, 1, gate, up, *moments)
        pieces = layers * PARTS
        down = pl.pallas_call(
            functools.partial(gather_last, n),
            out_shape=pltpu.VMEM(weights[2].shape, weights[2].dtype),
            in_specs=[vmem, vmem],
            out_specs=vmem,
            scratch_shapes=[
                pltpu.SemaphoreType.DMA((WAYS, pieces)),
                pltpu.SemaphoreType.DMA((WAYS, n - 1, pieces)),
            ],
            compiler_params=pltpu.CompilerParams(
                collective_id=1, has_side_effects=True, vmem_limit_bytes=24 * 2**20
            ),
            name="gather_last",
        )(own_down, token)
        (down,) = put(24, 0, down)
        return gate, up, down, *moments

    all_of, cut = P(None, None, None), P(None, "dp", None)
    return jax.shard_map(
        step,
        mesh=mesh,
        in_specs=(P(("rep", "dp"), None, None, None),) * 3 + (all_of,) * 3 + (cut,) * 6,
        out_specs=(P("rep", None, None),) * 3 + (P("rep", "dp", None),) * 6,
        check_vma=False,
    )
```
